16 devices in a mesh: data: 2 (over y, z), seq: 8 (over x, core).
Axes of the slice: x: 4, y: 2, z: 1, core: 2. Of those that a mesh axis runs over, the one named last changes fastest.
The devices are a block of a 4x4x8 slice.
Arguments:
- act_in: bfloat16 [128, 1024, 1024], P('data', 'seq'), parts along dimension 0
- grad_out: bfloat16 [128, 1024, 1024], P('data', 'seq'), parts along dimension 0
- ln1_scale: float32 [1024], replicated
- ln1_shift: float32 [1024], replicated
- w_tok1: bfloat16 [1024, 512], replicated
- b_tok1: float32 [512], replicated
- w_tok2: bfloat16 [512, 1024], replicated
- b_tok2: float32 [1024], replicated
- ln2_scale: float32 [1024], replicated
- ln2_shift: float32 [1024], replicated
- w_chan1: bfloat16 [1024, 4096], replicated
- b_chan1: float32 [4096], replicated
- w_chan2: bfloat16 [4096, 1024], replicated
- b_chan2: float32 [1024], replicated
Outputs:
- output 1: bfloat16 [128, 1024, 1024], P('data', 'seq'), parts along dimension 0
- output 2: bfloat16 [128, 1024, 1024], P('data', 'seq'), parts along dimension 0
- output 3: float32 [2048, 512], P('data'), parts along dimension 0
- output 4: float32 [1024, 1024], P('data'), parts along dimension 0
- output 5: float32 [2048, 4096], P('data'), parts along dimension 0
- output 6: float32 [8192, 1024], P('data'), parts along dimension 0
There are 2 independent parts. The reference program is written for one: setup_inputs(seed, part) draws one part's arguments, and reference() takes and returns one part's arrays. A program takes and returns all parts, laid end to end along the dimension named above; an argument that names none is the same for every part.
All inputs are finite; a program needn't handle non-finite values.
Results may differ from the reference program's by a relative error of at most 0.0164204.
Values are sent between devices in bfloat16 or wider.
A program may use at most 768 MiB of HBM per device.

```python
import jax
import jax.numpy as jnp
from jax import lax

IMAGES = 64
PATCHES = 1024
CHANNELS = 1024
TOKEN_HID = 512
CHAN_HID = 4096

LN_EPS = 1e-6


def setup_inputs(seed: int = 0, part: int = 0) -> dict:
    part_key = jax.random.fold_in(jax.random.key(seed), part)
    act_key, grad_key = jax.random.split(part_key)
    weight_keys = jax.random.split(jax.random.key(seed + 1), 12)

    def draw_normal(key_index, shape, spread):
        return jax.random.normal(weight_keys[key_index], shape, jnp.float32) * spread

    act_in = jax.random.normal(act_key, (IMAGES, PATCHES, CHANNELS), jnp.float32)
    grad_out = jax.random.normal(grad_key, (IMAGES, PATCHES, CHANNELS), jnp.float32)
    return {
        "act_in": act_in.astype(jnp.bfloat16),
        "grad_out": grad_out.astype(jnp.bfloat16),
        "ln1_scale": 1.0 + draw_normal(0, (CHANNELS,), 0.3),
        "ln1_shift": draw_normal(1, (CHANNELS,), 0.3),
        "w_tok1": draw_normal(2, (PATCHES, TOKEN_HID), PATCHES ** -0.5).astype(jnp.bfloat16),
        "b_tok1": draw_normal(3, (TOKEN_HID,), 0.5),
        "w_tok2": draw_normal(4, (TOKEN_HID, PATCHES), TOKEN_HID ** -0.5).astype(jnp.bfloat16),
        "b_tok2": draw_normal(5, (PATCHES,), 0.5),
        "ln2_scale": 1.0 + draw_normal(6, (CHANNELS,), 0.3),
        "ln2_shift": draw_normal(7, (CHANNELS,), 0.3),
        "w_chan1": draw_normal(8, (CHANNELS, CHAN_HID), CHANNELS ** -0.5).astype(jnp.bfloat16),
        "b_chan1": draw_normal(9, (CHAN_HID,), 0.5),
        "w_chan2": draw_normal(10, (CHAN_HID, CHANNELS), CHAN_HID ** -0.5).astype(jnp.bfloat16),
        "b_chan2": draw_normal(11, (CHANNELS,), 0.5),
    }


def layer_norm(rows_in, ln_scale, ln_shift):
    widened = rows_in.astype(jnp.float32)
    row_mean = jnp.mean(widened, axis=-1, keepdims=True)
    centered = widened - row_mean
    row_var = jnp.mean(centered * centered, axis=-1, keepdims=True)
    return (centered * lax.rsqrt(row_var + LN_EPS) * ln_scale + ln_shift).astype(jnp.bfloat16)


def gelu_bf16(pre_act):
    return jax.nn.gelu(pre_act.astype(jnp.float32)).astype(jnp.bfloat16)


def reference(act_in, grad_out, ln1_scale, ln1_shift, w_tok1, b_tok1, w_tok2, b_tok2,
              ln2_scale, ln2_shift, w_chan1, b_chan1, w_chan2, b_chan2):
    def layer_forward(tok1_wide, tok2_wide, chan1_wide, chan2_wide, image):
        normed = layer_norm(image, ln1_scale, ln1_shift)
        tok_pre = (jnp.einsum("sd,sc->dc", tok1_wide, normed.astype(jnp.float32))
                   + b_tok1[:, None]).astype(jnp.bfloat16)
        tok_act = gelu_bf16(tok_pre)
        tok_out = (jnp.einsum("ds,dc->sc", tok2_wide, tok_act.astype(jnp.float32))
                   + b_tok2[:, None]).astype(jnp.bfloat16)
        mid_act = (image.astype(jnp.float32) + tok_out.astype(jnp.float32)).astype(jnp.bfloat16)
        normed_mid = layer_norm(mid_act, ln2_scale, ln2_shift)
        chan_pre = (jnp.einsum("sc,ch->sh", normed_mid.astype(jnp.float32), chan1_wide)
                    + b_chan1).astype(jnp.bfloat16)
        chan_act = gelu_bf16(chan_pre)
        chan_out = jnp.einsum("sh,hc->sc", chan_act.astype(jnp.float32), chan2_wide) + b_chan2
        return (mid_act.astype(jnp.float32) + chan_out).astype(jnp.bfloat16)

    tok1_wide = w_tok1.astype(jnp.float32)
    tok2_wide = w_tok2.astype(jnp.float32)
    chan1_wide = w_chan1.astype(jnp.float32)
    chan2_wide = w_chan2.astype(jnp.float32)

    def image_step(grad_sums, image_pair):
        image, image_grad = image_pair
        image_out, pullback = jax.vjp(layer_forward, tok1_wide, tok2_wide, chan1_wide, chan2_wide, image)
        cotangents = pullback(image_grad)
        new_sums = tuple(total + piece for total, piece in zip(grad_sums, cotangents[:4]))
        return new_sums, (image_out, cotangents[4])

    zero_sums = (jnp.zeros(w_tok1.shape, jnp.float32), jnp.zeros(w_tok2.shape, jnp.float32),
                 jnp.zeros(w_chan1.shape, jnp.float32), jnp.zeros(w_chan2.shape, jnp.float32))
    weight_sums, (act_out, grad_in) = lax.scan(image_step, zero_sums, (act_in, grad_out))
    return act_out, grad_in, weight_sums[0], weight_sums[1], weight_sums[2], weight_sums[3]
```

```python
import functools
import math

import jax
import jax.numpy as jnp
from jax import lax
from jax.experimental import pallas as pl
from jax.experimental.pallas import tpu as pltpu
from jax.sharding import PartitionSpec as P

LN_EPS = 1e-6
GELU_C = math.sqrt(2.0 / math.pi)
F32, BF16 = jnp.float32, jnp.bfloat16
AHEAD = 3
ROWS_LN = 32
TILE = 512


def dot(a, b):
    return jnp.dot(a, b, preferred_element_type=F32)


def dot_nt(a, b):
    return lax.dot_general(a, b, (((1,), (1,)), ((), ())), preferred_element_type=F32)


def gelu(x):
    th = jnp.tanh(GELU_C * (x + 0.044715 * (x * x * x)))
    return 0.5 * x * (1.0 + th)


def gelu_and_slope(x):
    sq = x * x
    th = jnp.tanh(x * (GELU_C + (GELU_C * 0.044715) * sq))
    half = 0.5 + 0.5 * th
    slope = half + (0.5 * x) * (1.0 - th * th) * (GELU_C + (3.0 * 0.044715 * GELU_C) * sq)
    return x * half, slope


def normalize(rows_in):
    mean = jnp.mean(rows_in, axis=-1, keepdims=True)
    centered = rows_in - mean
    inv = lax.rsqrt(jnp.mean(centered * centered, axis=-1, keepdims=True) + LN_EPS)
    return centered * inv, inv


def norm_grad(unit, inv, scaled):
    return inv * (scaled - jnp.mean(scaled, axis=-1, keepdims=True)
                  - unit * jnp.mean(scaled * unit, axis=-1, keepdims=True))


def layer_kernel(n, x_hbm, dz_hbm, s1, o1, s2, o2, bt1, bt2, b1_ref, b2_ref, wt1, wt1_t, wt2, wt2_t, wc1, wc2, eye,
                 z_out, dx_out, dw1_hbm, dw2_hbm, dwt1, dwt2, xg, dzg, zg, dxg,
                 xv, dzv, x1, v, h, g, vt, dzt, zacc, dvacc, q, da, w1s, w2s, d1s, d2s,
                 send_in, send_out, recv_x, recv_dz, recv_z, recv_dx, load_x, load_dz, store, own_out, wsem, dsem_in, dsem_out):
    me = lax.axis_index("seq")
    own, rows, chans = x_hbm.shape[0] // n, x_hbm.shape[1], x_hbm.shape[2]
    patches = n * rows
    hid_tok = h.shape[0]
    hid = wc1.shape[1]
    block = w1s.shape[2]
    blocks = hid // block
    steps = own * blocks

    def peer(k):
        return lax.rem(me + k, n)

    def rsl(i, size):
        return pl.ds(pl.multiple_of(i * size, size), size)

    barrier = pltpu.get_barrier_semaphore()
    for k in range(1, n):
        pl.semaphore_signal(barrier, inc=1, device_id={"seq": peer(k)}, device_id_type=pl.DeviceIdType.MESH)
    pl.semaphore_wait(barrier, n - 1)

    def send_image(i):
        for src, dst, recv, idx in ((x_hbm, xg, recv_x, 0), (dz_hbm, dzg, recv_dz, 1)):
            for k in range(1, n):
                p = peer(k)
                pltpu.make_async_remote_copy(
                    src_ref=src.at[p * own + i], dst_ref=dst.at[i, me], send_sem=send_in.at[idx], recv_sem=recv.at[i],
                    device_id={"seq": p}, device_id_type=pl.DeviceIdType.MESH).start()

    def send_result(i):
        for src, dst, recv, idx in ((zg, z_out, recv_z, 0), (dxg, dx_out, recv_dx, 1)):
            for k in range(1, n):
                p = peer(k)
                pltpu.make_async_remote_copy(
                    src_ref=src.at[i, p], dst_ref=dst.at[me * own + i], send_sem=send_out.at[idx], recv_sem=recv.at[0],
                    device_id={"seq": p}, device_id_type=pl.DeviceIdType.MESH).start()

    def wait_bytes(ref, sem):
        pltpu.make_async_copy(ref, ref, sem).wait()

    def load_image(i, src, gathered, buf, recv, sem):
        wait_bytes(gathered.at[0, pl.ds(0, n - 1)], recv.at[i])
        for k in range(n):
            p = peer(k)
            ref = src.at[me * own + i] if k == 0 else gathered.at[i, p]
            pltpu.make_async_copy(ref, buf.at[rsl(p, rows)], sem).start()

    def weight_copies(t):
        j, slot = lax.rem(t, blocks), lax.rem(t, 2)
        return (pltpu.make_async_copy(wc1.at[:, rsl(j, block)], w1s.at[slot], wsem.at[0, slot]),
                pltpu.make_async_copy(wc2.at[rsl(j, block)], w2s.at[slot], wsem.at[1, slot]))

    def grad_refs(t):
        j, slot = lax.rem(t, blocks), lax.rem(t, 3)
        return ((dw1_hbm.at[:, rsl(j, block)], d1s.at[slot]), (dw2_hbm.at[:, rsl(j, block)], d2s.at[slot]))

    def grad_in(t):
        return [pltpu.make_async_copy(a, b, dsem_in.at[m, lax.rem(t, 3)]) for m, (a, b) in enumerate(grad_refs(t))]

    def grad_out(t):
        return [pltpu.make_async_copy(b, a, dsem_out.at[m, lax.rem(t, 3)]) for m, (a, b) in enumerate(grad_refs(t))]

    def result_copies(i):
        out = []
        for m, (buf, staged, final) in enumerate(((x1, zg, z_out), (dzt, dxg, dx_out))):
            out.append(pltpu.make_async_copy(buf.at[rsl(me, rows)], final.at[me * own + i], own_out.at[m]))
            for k in range(1, n):
                p = peer(k)
                out.append(pltpu.make_async_copy(buf.at[rsl(p, rows)], staged.at[i, p], store.at[m]))
        return out

    def wait_results():
        for m in range(2):
            wait_bytes(zg.at[0, pl.ds(0, n - 1)], store.at[m])
            wait_bytes(zg.at[0, 0], own_out.at[m])

    for i in range(min(AHEAD, own)):
        send_image(i)
    for c in weight_copies(0):
        c.start()
    dwt1[...] = jnp.zeros_like(dwt1)
    dwt2[...] = jnp.zeros_like(dwt2)
    load_image(0, x_hbm, xg, xv.at[0], recv_x, load_x.at[0])

    def image_step(i, carry):
        slot = lax.rem(i, 2)
        xi = xv.at[slot]

        @pl.when(i + AHEAD < own)
        def _():
            send_image(i + AHEAD)

        @pl.when(i > 0)
        def _():
            wait_results()
            send_result(i - 1)

        wait_bytes(xi, load_x.at[slot])

        def ln1_rows(r, c):
            sl = rsl(r, ROWS_LN)
            unit, _ = normalize(xi[sl].astype(F32))
            vt[sl] = (unit * s1[...] + o1[...]).astype(BF16)
            return c

        lax.fori_loop(0, patches // ROWS_LN, ln1_rows, 0)

        def tok_hidden(ct, c):
            sl = rsl(ct, TILE)
            pre = (dot(wt1_t[...], vt[:, sl]) + bt1[...]).astype(BF16)
            h[:, sl] = pre
            g[:, sl] = gelu(pre.astype(F32)).astype(BF16)
            return c

        lax.fori_loop(0, chans // TILE, tok_hidden, 0)
        load_image(i, dz_hbm, dzg, dzv, recv_dz, load_dz)

        def tok_out(rt, c):
            sl = rsl(rt, TILE)
            t = (dot(wt2_t[sl], g[...]) + bt2[sl]).astype(BF16)
            mid = (xi[sl].astype(F32) + t.astype(F32)).astype(BF16)
            x1[sl] = mid
            return c

        lax.fori_loop(0, patches // TILE, tok_out, 0)

        def ln2_rows(r, c):
            sl = rsl(r, ROWS_LN)
            mid = x1[sl].astype(F32)
            unit, _ = normalize(mid)
            v[sl] = (unit * s2[...] + o2[...]).astype(BF16)
            zacc[sl] = mid + b2_ref[...]
            dvacc[sl] = jnp.zeros_like(mid)
            return c

        lax.fori_loop(0, patches // ROWS_LN, ln2_rows, 0)
        wait_bytes(dzv, load_dz)

        def flip(ct, c):
            sl = rsl(ct, 256)
            vt[sl] = dot_nt(eye[...], v[:, sl]).astype(BF16)
            dzt[sl] = dot_nt(eye[...], dzv[:, sl]).astype(BF16)
            return c

        lax.fori_loop(0, chans // 256, flip, 0)

        def chan_step(j, c):
            t = i * blocks + j
            ws, ds = lax.rem(t, 2), lax.rem(t, 3)
            for cp in weight_copies(t):
                cp.wait()

            @pl.when(t + 1 < steps)
            def _():
                for cp in weight_copies(t + 1):
                    cp.start()

            @pl.when(t >= 2)
            def _():
                for cp in grad_out(t - 2):
                    cp.wait()

            @pl.when(jnp.logical_and(t + 1 >= blocks, t + 1 < steps))
            def _():
                for cp in grad_in(t + 1):
                    cp.start()

            bias = b1_ref[:, rsl(j, block)]

            def rows_step(rt, c2):
                sl = rsl(rt, TILE)
                a = (dot(v[sl], w1s[ws]) + bias).astype(BF16)
                act, slope = gelu_and_slope(a.astype(F32))
                act = act.astype(BF16)
                q[sl] = act
                dq = dot_nt(dzv[sl], w2s[ws]).astype(BF16)
                grad = (dq.astype(F32) * slope).astype(BF16)
                da[sl] = grad
                zacc[sl] += dot(act, w2s[ws])
                dvacc[sl] += dot_nt(grad, w1s[ws])
                return c2

            lax.fori_loop(0, patches // TILE, rows_step, 0)

            @pl.when(i == 0)
            def _():
                d1s[ds] = jnp.zeros(d1s.shape[1:], F32)
                d2s[ds] = jnp.zeros(d2s.shape[1:], F32)

            @pl.when(i > 0)
            def _():
                for cp in grad_in(t):
                    cp.wait()

            def weights_step(rt, c2):
                sl = rsl(rt, TILE)
                d1s[ds, sl] += dot(vt[sl], da[...])
                d2s[ds, sl] += dot(dzt[sl], q[...])
                return c2

            lax.fori_loop(0, chans // TILE, weights_step, 0)
            for cp in grad_out(t):
                cp.start()
            return c

        lax.fori_loop(0, blocks, chan_step, 0)

        @pl.when(i + 1 < own)
        def _():
            load_image(i + 1, x_hbm, xg, xv.at[1 - slot], recv_x, load_x.at[1 - slot])

        def ln2_grad(r, c):
            sl = rsl(r, ROWS_LN)
            unit, inv = normalize(x1[sl].astype(F32))
            scaled = dvacc[sl].astype(BF16).astype(F32) * s2[...]
            through = norm_grad(unit, inv, scaled).astype(BF16)
            v[sl] = (dzv[sl].astype(F32) + through.astype(F32)).astype(BF16)
            x1[sl] = zacc[sl].astype(BF16)
            unit1, _ = normalize(xi[sl].astype(F32))
            vt[sl] = (unit1 * s1[...] + o1[...]).astype(BF16)
            return c

        lax.fori_loop(0, patches // ROWS_LN, ln2_grad, 0)

        def tok_hidden_grad(ct, c):
            sl = rsl(ct, TILE)
            dg = dot(wt2[...], v[:, sl]).astype(BF16)
            _, slope = gelu_and_slope(h[:, sl].astype(F32))
            h[:, sl] = (dg.astype(F32) * slope).astype(BF16)
            return c

        lax.fori_loop(0, chans // TILE, tok_hidden_grad, 0)

        def tok_weights(rt, c):
            sl = rsl(rt, TILE)
            dwt1[sl] += dot_nt(vt[sl], h[...])
            dwt2[:, sl] += dot_nt(g[...], v[sl])
            return c

        lax.fori_loop(0, patches // TILE, tok_weights, 0)

        def tok_in_grad(rt, c):
            sl = rsl(rt, TILE)
            vt[sl] = dot(wt1[sl], h[...]).astype(BF16)
            return c

        lax.fori_loop(0, patches // TILE, tok_in_grad, 0)

        def ln1_grad(r, c):
            sl = rsl(r, ROWS_LN)
            unit, inv = normalize(xi[sl].astype(F32))
            through = norm_grad(unit, inv, vt[sl].astype(F32) * s1[...]).astype(BF16)
            dzt[sl] = (v[sl].astype(F32) + through.astype(F32)).astype(BF16)
            return c

        lax.fori_loop(0, patches // ROWS_LN, ln1_grad, 0)
        for cp in result_copies(i):
            cp.start()
        return carry

    lax.fori_loop(0, own, image_step, 0)
    for t in (steps - 2, steps - 1):
        for cp in grad_out(t):
            cp.wait()
    wait_results()
    send_result(own - 1)
    for m in range(2):
        wait_bytes(xg.at[:, pl.ds(0, n - 1)], send_in.at[m])
        wait_bytes(xg.at[:, pl.ds(0, n - 1)], send_out.at[m])
    wait_bytes(xg.at[:, pl.ds(0, n - 1)], recv_z.at[0])
    wait_bytes(xg.at[:, pl.ds(0, n - 1)], recv_dx.at[0])


def solution(mesh):
    act_spec = P("data", "seq", None)
    part_spec = P("data", None)
    spec_in = (act_spec, act_spec) + (P(),) * 12
    spec_out = (act_spec, act_spec, part_spec, part_spec, part_spec, part_spec)
    n = mesh.shape["seq"]

    def device_step(act_loc, grad_loc, ln1_scale, ln1_shift, w_tok1, b_tok1, w_tok2, b_tok2,
                    ln2_scale, ln2_shift, w_chan1, b_chan1, w_chan2, b_chan2):
        images, rows, chans = act_loc.shape
        own, patches = images // n, rows * n
        hid_tok, hid = w_tok1.shape[1], w_chan1.shape[1]
        block = 512
        vm, hbm = pl.BlockSpec(memory_space=pltpu.VMEM), pl.BlockSpec(memory_space=pl.ANY)
        act_shape = jax.ShapeDtypeStruct(act_loc.shape, BF16)
        stage = jax.ShapeDtypeStruct((own, n, rows, chans), BF16)
        dma = pltpu.SemaphoreType.DMA
        flops = 12 * own * patches * chans * (hid + hid_tok)
        outs = pl.pallas_call(
            functools.partial(layer_kernel, n),
            out_shape=(act_shape, act_shape, jax.ShapeDtypeStruct((chans, hid), F32), jax.ShapeDtypeStruct((chans, hid), F32),
                       jax.ShapeDtypeStruct((patches, hid_tok), F32), jax.ShapeDtypeStruct((hid_tok, patches), F32),
                       stage, stage, stage, stage),
            in_specs=[hbm, hbm] + [vm] * 12 + [hbm, hbm, vm],
            out_specs=(hbm, hbm, hbm, hbm, vm, vm, hbm, hbm, hbm, hbm),
            scratch_shapes=[
                pltpu.VMEM((2, patches, chans), BF16), pltpu.VMEM((patches, chans), BF16),
                pltpu.VMEM((patches, chans), BF16), pltpu.VMEM((patches, chans), BF16),
                pltpu.VMEM((hid_tok, chans), BF16), pltpu.VMEM((hid_tok, chans), BF16),
                pltpu.VMEM((patches, chans), BF16), pltpu.VMEM((patches, chans), BF16),
                pltpu.VMEM((patches, chans), F32), pltpu.VMEM((patches, chans), F32),
                pltpu.VMEM((patches, block), BF16), pltpu.VMEM((patches, block), BF16),
                pltpu.VMEM((2, chans, block), BF16), pltpu.VMEM((2, block, chans), BF16),
                pltpu.VMEM((3, chans, block), F32), pltpu.VMEM((3, chans, block), F32),
                dma((2,)), dma((2,)), dma((own,)), dma((own,)), dma((1,)), dma((1,)),
                dma((2,)), dma, dma((2,)), dma((2,)), dma((2, 2)), dma((2, 3)), dma((2, 3)),
            ],
            compiler_params=pltpu.CompilerParams(
                collective_id=0, has_side_effects=True, vmem_limit_bytes=67_000_000),
            cost_estimate=pl.CostEstimate(flops=flops, bytes_accessed=10 * act_loc.size, transcendentals=0),
        )(act_loc, grad_loc, ln1_scale[None], ln1_shift[None], ln2_scale[None], ln2_shift[None], b_tok1[:, None],
          b_tok2[:, None], b_chan1[None], b_chan2[None], w_tok1, w_tok1.T, w_tok2, w_tok2.T, w_chan1, w_chan2,
          jnp.eye(256, dtype=BF16))
        act_out, grad_in, dw1, dw2_t, dwt1, dwt2 = outs[:6]
        grads = lax.psum((dwt1, dwt2, dw1, dw2_t.T), "seq")
        return (act_out, grad_in) + tuple(grads)

    return jax.shard_map(device_step, mesh=mesh, in_specs=spec_in, out_specs=spec_out, check_vma=False)
```
